32 devices in a mesh: ctx: 16 (over z, y, core), tp: 2 (over x).
Axes of the slice: x: 2, y: 2, z: 4, core: 2. Of those that a mesh axis runs over, the one named last changes fastest.
Arguments:
- tokens: bfloat16 [4096, 8192], P(('ctx', 'tp')), may hold values from -64 to 64
- query_weight: bfloat16 [8192, 1024], P(None, 'tp'), may hold values from -0.0625 to 0.0625
- keyval_weight: bfloat16 [8192, 512], P(None, 'tp'), may hold values from -0.0625 to 0.0625
- doc_lengths: int32 [32], replicated, may hold values from 1 to 2048, 4096 in all
- owners: int32 [128], replicated, may hold values from 0 to 15, as said below
Outputs:
- attended: bfloat16 [4096, 1024], P('ctx', 'tp')
The draws below stay inside these ranges and needn't reach their ends.
Inputs may be any that keep to these rules, and one draw needn't show every extreme that they name: The 8 blocks of one index of ctx (blocks i * 8 to (i + 1) * 8 - 1) go to 8 different owners; for each position j < 8, the blocks i * 8 + j of all indices i go to all different owners, so every owner receives exactly one block of each position.
All inputs are finite; a program needn't handle non-finite values.
Results may differ from the reference program's by a relative error of at most 0.0055.
The reference program's roundings to bfloat16 on the way count: a program that leaves them out, or rounds other values in their place, can miss the bound.
Values may be sent and summed in bfloat16 or wider, within the bound.
No kernel may reach another device: no remote copies, remote signals or barrier semaphores. Data moves between devices by JAX's collectives and lax.ppermute only.
A program may use at most 128 MiB of HBM per device.

```python
import math
import jax
import jax.numpy as jnp
import numpy as np
from jax import lax

D = 8192
HD = 128
HEADS = 4
QW = 1024
TOKENS = 4096
BLOCKS_DEV = 8
BLOCKS = 128
NDOC = 32
DOC_MOST = 2048
N_TP = 2


def draw_tokens(key, part):
    first = jax.random.fold_in(jax.random.fold_in(key, 7), 0)
    values = jnp.clip(jax.random.normal(first, (TOKENS, D), jnp.float32), -6.0, 6.0)
    return values.astype(jnp.bfloat16)


def draw_owners(key, part):
    cycle_count = BLOCKS // BLOCKS_DEV
    first, second = jax.random.split(jax.random.fold_in(key, 11))
    shuffle = jax.random.permutation(first, cycle_count)
    inverse = jnp.argsort(shuffle)
    offsets = jax.random.permutation(second, cycle_count)[:BLOCKS_DEV]
    chosen = shuffle[(inverse[:, None] + offsets[None, :]) % cycle_count]
    return chosen.reshape(BLOCKS).astype(jnp.int32)


def level_of(rng, shape, cuts, least, high):
    factor_of = 1.0
    for position, shards_of in cuts:
        heights = jax.random.uniform(jax.random.fold_in(jax.random.fold_in(rng, 6), position), (shards_of,), jnp.float32, least / len(cuts), high / len(cuts))
        factor_of = factor_of * jnp.repeat(jnp.exp(heights), shape[position] // shards_of).reshape((-1,) + (1,) * (len(shape) - 1 - position))
    return factor_of


def length_profile(count, total, limit, slope):
    loads = [(1 << 20) // math.isqrt(standing ** slope) + 1 for standing in range(2, count + 1)]
    surplus, counts = total - limit - (count - 1), [1] * (count - 1)
    while surplus > 0:
        movable = [i for i in range(count - 1) if counts[i] < limit]
        mass, budget = sum([loads[i] for i in movable]), surplus
        for i in movable:
            more = min(limit - counts[i], max(1, budget * loads[i] // mass), surplus)
            counts[i] = counts[i] + more
            surplus = surplus - more
    return np.array([limit] + counts)


def ragged(key, number_of, total, most, skew):
    if number_of == 2:
        one = jax.random.randint(key, (), max(1, total - most), min(most, total - 1) + 1)
        return jnp.stack([one, total - one])
    lengths = jnp.asarray(length_profile(number_of, total, most, skew), jnp.int32)
    pairs = (number_of - 1) // 2
    giver, sink = lengths[1:1 + 2 * pairs:2], lengths[2:2 + 2 * pairs:2]
    margin = jnp.minimum(giver - 1, most - sink)
    shifted = jax.random.randint(jax.random.fold_in(key, 1), (pairs,), 0, 1 << 20) % (margin + 1)
    lengths = lengths.at[1:1 + 2 * pairs:2].set(giver - shifted).at[2:2 + 2 * pairs:2].set(sink + shifted)
    return lengths[jax.random.permutation(jax.random.fold_in(key, 2), number_of)]


def bell_draw(stream_key, shape, deviation, bound, shards=(), held_as=jnp.bfloat16):
    level = level_of(stream_key, shape, shards, -0.22, 0.18) if shards else 1.0
    array = jax.random.normal(stream_key, shape, jnp.float32) * deviation * level
    return jnp.minimum(jnp.maximum(array, -bound), bound).astype(held_as)


def setup_inputs(seed: int = 0) -> dict:
    streams_of = jax.random.split(jax.random.key(seed), 6)
    return {
        "tokens": draw_tokens(jax.random.fold_in(streams_of[5], 71), 0),
        "query_weight": bell_draw(streams_of[1], (D, QW), D ** -0.5, 0.0625, ((1, 2),)),
        "keyval_weight": bell_draw(streams_of[2], (D, 2 * HD * N_TP), D ** -0.5, 0.0625, ((1, 2),)),
        "doc_lengths": ragged(streams_of[3], NDOC, TOKENS, DOC_MOST, 2).astype(jnp.int32),
        "owners": draw_owners(jax.random.fold_in(streams_of[5], 71), 0),
    }


NEG_FILL = -1e+30

def reference(tokens, query_weight, keyval_weight, doc_lengths, owners):
    total = tokens.shape[0]
    head_dim = HD
    heads = HEADS
    queries = jnp.dot(tokens, query_weight, preferred_element_type=jnp.float32).astype(jnp.bfloat16)
    keyvals = jnp.dot(tokens, keyval_weight, preferred_element_type=jnp.float32).astype(jnp.bfloat16)
    doc_ends = jnp.cumsum(doc_lengths).astype(jnp.int32)
    token_place = jnp.arange(total, dtype=jnp.int32)
    token_docs = lax.optimization_barrier(jnp.sum((doc_ends[None, :] <= token_place[:, None]).astype(jnp.int32), axis=1))
    block_rows = math.gcd(total, 512)
    score_scale = 1.0 / math.sqrt(head_dim)
    starts = jnp.arange(total // block_rows, dtype=jnp.int32) * block_rows
    outputs = []
    for group in range(N_TP):
        group_queries = queries[:, group * heads * head_dim:(group + 1) * heads * head_dim]
        key_rows = keyvals[:, 2 * head_dim * group:2 * head_dim * group + head_dim].astype(jnp.float32)
        value_rows = keyvals[:, 2 * head_dim * group + head_dim:2 * head_dim * (group + 1)].astype(jnp.float32)

        def attend(first_row):
            query_rows = lax.dynamic_slice_in_dim(group_queries, first_row, block_rows, 0).astype(jnp.float32)
            query_rows = query_rows.reshape(block_rows, heads, head_dim)
            query_place = lax.dynamic_slice_in_dim(token_place, first_row, block_rows, 0)
            query_docs = lax.dynamic_slice_in_dim(token_docs, first_row, block_rows, 0)
            allowed = (query_docs[:, None] == token_docs[None, :]) & (token_place[None, :] <= query_place[:, None])
            scores = jnp.einsum('qhd,kd->hqk', query_rows, key_rows) * score_scale
            scores = jnp.where(allowed[None], scores, NEG_FILL)
            highest = lax.optimization_barrier(jnp.max(scores, axis=2))
            weights = jnp.where(allowed[None], jnp.exp(scores - highest[:, :, None]), 0.0)
            totals = lax.optimization_barrier(jnp.sum(weights, axis=2))
            rounded = weights.astype(jnp.bfloat16).astype(jnp.float32)
            summed = jnp.einsum('hqk,kd->hqd', rounded, value_rows)
            result = summed / totals[:, :, None]
            return result.transpose(1, 0, 2).reshape(block_rows, heads * head_dim).astype(jnp.bfloat16)
        outputs.append(lax.map(attend, starts).reshape(total, heads * head_dim))
    head_out = jnp.concatenate(outputs, axis=1)
    block_count = owners.shape[0]
    block_len = total // block_count
    block_order = jnp.argsort(owners, stable=True).astype(jnp.int32)
    row_index = (block_order[:, None] * block_len + jnp.arange(block_len, dtype=jnp.int32)[None, :]).reshape(total)
    return head_out[row_index]
```

```python
import functools
import math

import jax
import jax.numpy as jnp
from jax import lax
from jax.experimental import pallas as pl
from jax.experimental.pallas import tpu as pltpu
from jax.sharding import PartitionSpec as P


NEG_FILL = -1e30
LOG2E = 1.4426950408889634
UNROLL = 4


def project(rows, query_weight, keyval_weight):
    query = jnp.dot(rows, query_weight, preferred_element_type=jnp.float32)
    keyval = jnp.dot(rows, keyval_weight, preferred_element_type=jnp.float32)
    return query.astype(jnp.bfloat16), keyval.astype(jnp.bfloat16)


def gather_bits(count):
    bits = [1 << b for b in range(count.bit_length() - 1)]
    return bits[1:] + bits[:1]


def gather_all(part, count):
    held = part[None]
    for bit in gather_bits(count):
        pairs = [(i, i ^ bit) for i in range(count)]
        held = jnp.concatenate([held, lax.ppermute(held, "ctx", pairs)], axis=0)
    return held


def slot_source(slot, me, count):
    code = 0
    for place, bit in enumerate(gather_bits(count)):
        if slot >> place & 1:
            code |= bit
    return me ^ code


def source_slot(source, me, count):
    differ = source ^ me
    slot = 0
    for place, bit in enumerate(gather_bits(count)):
        slot = slot + ((differ // bit) % 2) * (1 << place)
    return slot


def attend_kernel(
    count,
    heads,
    segments,
    info_ref,
    source_ref,
    slot_ref,
    rank_ref,
    item_block_ref,
    item_tile_ref,
    start_ref,
    place_ref,
    arrived_ref,
    late_ref,
    *rest,
):
    keyval_refs = rest[: len(segments) - 1]
    out_ref, key_ref, value_ref, valt_ref, query_ref, max_ref, sum_ref, acc_ref = rest[
        len(segments) - 1 :
    ]
    blocks, per_block = start_ref.shape
    block_len = arrived_ref.shape[1]
    dim = key_ref.shape[2]
    rows = key_ref.shape[1]
    query_cols = heads * dim
    me = info_ref[0]
    late_place = info_ref[1]
    iterations = info_ref[2]

    for index, (offset_at, first, length) in enumerate(segments):
        row = pl.multiple_of(info_ref[offset_at] + first, math.gcd(first, 16) if first else 16)
        last = index == len(segments) - 1
        for slot in range(count):
            source = slot_source(slot, me, count)
            if last:
                piece = late_ref[slot, :, query_cols:]
            else:
                piece = keyval_refs[index][slot]
            key_ref[source, pl.ds(row, length), :] = piece[:, :dim]
            value_ref[source, pl.ds(row, length), :] = piece[:, dim:]
    for tile in range(count):
        valt_ref[tile] = value_ref[tile].T

    for block in range(blocks):

        @pl.when(block == late_place)
        def _():
            slot = slot_ref[block]
            for head in range(heads):
                query_ref[block, head * block_len : (head + 1) * block_len, :] = late_ref[
                    slot, :, head * dim : (head + 1) * dim
                ]

        @pl.when(block != late_place)
        def _():
            source = source_ref[block]
            for head in range(heads):
                query_ref[block, head * block_len : (head + 1) * block_len, :] = arrived_ref[
                    source, :, head * dim : (head + 1) * dim
                ]

    max_ref[...] = jnp.full_like(max_ref, NEG_FILL)
    sum_ref[...] = jnp.zeros_like(sum_ref)
    acc_ref[...] = jnp.zeros_like(acc_ref)
    key_index = lax.broadcasted_iota(jnp.int32, (rows, per_block), 0)
    scale = LOG2E / math.sqrt(dim)

    def step(iteration, carry):
        done = []
        for u in range(UNROLL):
            item = iteration * UNROLL + u
            block = item_block_ref[item]
            tile = item_tile_ref[item]
            safe = jnp.minimum(block, blocks - 1)
            scores = lax.dot_general(
                key_ref[tile],
                query_ref[safe],
                (((1,), (1,)), ((), ())),
                preferred_element_type=jnp.float32,
            )
            base = tile * rows
            start = start_ref[pl.ds(safe, 1), :] - base
            place = place_ref[pl.ds(safe, 1), :] - base
            allowed = (key_index >= start) & (key_index <= place)
            scores = jnp.where(allowed, scores * scale, NEG_FILL)
            highest = jnp.max(scores, axis=0, keepdims=True)
            weights = jnp.exp2(scores - highest)
            total = jnp.sum(weights, axis=0, keepdims=True)
            summed = lax.dot_general(
                valt_ref[tile],
                weights.astype(jnp.bfloat16),
                (((1,), (0,)), ((), ())),
                preferred_element_type=jnp.float32,
            )
            done.append((block, highest, total, summed))
        for block, highest, total, summed in done:
            old = max_ref[pl.ds(block, 1), :]
            new = jnp.maximum(old, highest)
            keep = jnp.exp2(old - new)
            add = jnp.exp2(highest - new)
            max_ref[pl.ds(block, 1), :] = new
            sum_ref[pl.ds(block, 1), :] = sum_ref[pl.ds(block, 1), :] * keep + total * add
            acc_ref[block] = acc_ref[block] * keep + summed * add
        return carry

    lax.fori_loop(0, iterations, step, 0)

    for block in range(blocks):
        result = (acc_ref[block] / sum_ref[block : block + 1, :]).T.astype(jnp.bfloat16)
        row = pl.multiple_of(rank_ref[block] * block_len, block_len)
        for head in range(heads):
            out_ref[pl.ds(row, block_len), head * dim : (head + 1) * dim] = result[
                head * block_len : (head + 1) * block_len, :
            ]


def body(tokens, query_weight, keyval_weight, doc_lengths, owners):
    count = lax.axis_size("ctx")
    me = lax.axis_index("ctx")
    groups = lax.axis_size("tp")
    member = lax.axis_index("tp")
    share = tokens.shape[0]
    rows = share * groups
    per = owners.shape[0] // count
    block_len = rows // per
    dim = keyval_weight.shape[1] // 2
    query_cols = query_weight.shape[1]
    heads = query_cols // dim
    share_blocks = share // block_len
    late = block_len
    weights = (query_weight, keyval_weight)

    pieces = []
    for shift in range(1, groups):
        if shift < groups - 1:
            pieces.append((shift, 0, share))
        else:
            if share > late:
                pieces.append((shift, 0, share - late))
            pieces.append((shift, share - late, late))
    arriving = []
    for shift, first, length in pieces:
        pairs = [(i, (i + shift) % groups) for i in range(groups)]
        arriving.append(lax.ppermute(tokens[first : first + length], "tp", pairs))

    grid = owners.reshape(count, per)
    place_of = jnp.arange(per, dtype=jnp.int32)
    sources = jnp.sum(
        jnp.where(grid == me, jnp.arange(count, dtype=jnp.int32)[:, None], 0), axis=0
    )
    mine = sources * per + place_of
    rank = jnp.sum((mine[None, :] < mine[:, None]).astype(jnp.int32), axis=1)
    length_count = doc_lengths.shape[0]
    order = jnp.arange(length_count)
    doc_ends = jnp.sum(
        jnp.where(order[None, :] <= order[:, None], doc_lengths[None, :], 0), axis=1
    )
    row_place = mine[:, None] * block_len + jnp.arange(block_len, dtype=jnp.int32)[None, :]
    row_start = jnp.max(
        jnp.where(doc_ends[None, None, :] <= row_place[:, :, None], doc_ends, 0), axis=2
    )
    first_tile = row_start[:, 0] // rows
    last_tile = row_place[:, -1] // rows
    tiles = last_tile - first_tile + 1
    before = jnp.sum(
        jnp.where(place_of[None, :] < place_of[:, None], tiles[None, :], 0), axis=1
    )
    item = jnp.arange(per * count + UNROLL, dtype=jnp.int32)
    within = (item[:, None] >= before[None, :]) & (item[:, None] < (before + tiles)[None, :])
    item_block = per - jnp.sum(jnp.where(within, per - place_of[None, :], 0), axis=1)
    item_tile = jnp.sum(
        jnp.where(within, first_tile[None, :] + item[:, None] - before[None, :], 0), axis=1
    )
    iterations = (jnp.sum(tiles) + UNROLL - 1) // UNROLL
    late_place = ((member + 1) % groups) * share_blocks + share_blocks - 1

    held_place = [member * share_blocks + j for j in range(share_blocks)]
    for shift, first, length in pieces[:-1]:
        begin = ((member - shift) % groups) * share_blocks
        held_place += [begin + (first // block_len) + j for j in range(length // block_len)]
    held_place = jnp.stack(held_place)
    own_targets = lax.dynamic_index_in_dim(grid, me, 0, keepdims=False)
    held_target = own_targets[held_place]
    held_index = jnp.arange(held_target.shape[0], dtype=jnp.int32)
    send_from = jnp.sum(
        jnp.where(
            held_target[None, :] == jnp.arange(count, dtype=jnp.int32)[:, None], held_index, 0
        ),
        axis=1,
    )

    own_query, own_keyval = project(tokens, *weights)
    gathered = [gather_all(own_keyval, count)]
    segments = [(3, 0, share)]
    offsets = [member * share]
    queries = [own_query]
    for index, (shift, first, length) in enumerate(pieces[:-1]):
        part_query, part_keyval = project(arriving[index], *weights)
        queries.append(part_query)
        gathered.append(gather_all(part_keyval, count))
        segments.append((3 + len(offsets), first, length))
        offsets.append(((member - shift) % groups) * share)
    held = jnp.concatenate(queries, axis=0).reshape(-1, block_len, query_cols)
    arrived = lax.all_to_all(held[send_from], "ctx", 0, 0, tiled=True)
    shift, first, length = pieces[-1]
    late_query, late_keyval = project(arriving[-1], *weights)
    gathered_late = gather_all(jnp.concatenate([late_query, late_keyval], axis=1), count)
    segments.append((3 + len(offsets), first, length))
    offsets.append(((member - shift) % groups) * share)

    info = jnp.stack([me, late_place, iterations, *offsets]).astype(jnp.int32)
    slots = source_slot(sources, me, count)
    per_block = heads * block_len
    smem = pl.BlockSpec(memory_space=pltpu.SMEM)
    vmem = pl.BlockSpec(memory_space=pltpu.VMEM)
    return pl.pallas_call(
        functools.partial(attend_kernel, count, heads, tuple(segments)),
        out_shape=jax.ShapeDtypeStruct((rows, query_cols), jnp.bfloat16),
        in_specs=[smem] * 6 + [vmem] * (4 + len(gathered)),
        out_specs=vmem,
        scratch_shapes=[
            pltpu.VMEM((count, rows, dim), jnp.bfloat16),
            pltpu.VMEM((count, rows, dim), jnp.bfloat16),
            pltpu.VMEM((count, dim, rows), jnp.bfloat16),
            pltpu.VMEM((per, per_block, dim), jnp.bfloat16),
            pltpu.VMEM((per + 1, per_block), jnp.float32),
            pltpu.VMEM((per + 1, per_block), jnp.float32),
            pltpu.VMEM((per + 1, dim, per_block), jnp.float32),
        ],
        name="attend",
    )(
        info,
        sources,
        slots,
        rank,
        item_block,
        item_tile,
        jnp.tile(row_start, (1, heads)),
        jnp.tile(row_place, (1, heads)),
        arrived,
        gathered_late,
        *gathered,
    )


def solution(mesh):
    return jax.shard_map(
        body,
        mesh=mesh,
        in_specs=(P(("ctx", "tp"), None), P(None, "tp"), P(None, "tp"), P(), P()),
        out_specs=P("ctx", "tp"),
        check_vma=False,
    )
```

```python
import functools
import math

import jax
import jax.numpy as jnp
from jax import lax
from jax.experimental import pallas as pl
from jax.experimental.pallas import tpu as pltpu
from jax.sharding import PartitionSpec as P


NEG_FILL = -1e30
LOG2E = 1.4426950408889634
UNROLL = 8


def route(queries, target_ref, send_ref):
    block_len = send_ref.shape[1]
    block = 0
    for query in queries:
        for first in range(0, query.shape[0], block_len):
            send_ref[target_ref[block]] = query[first : first + block_len]
            block += 1


def fetched_product(rows_ref, weights, stages, accs, sems):
    chunks = sems.shape[0]
    step = rows_ref.shape[1] // chunks

    def fetches(chunk):
        at = pl.ds(chunk * step, step)
        return [
            pltpu.make_async_copy(weight.at[at], stage.at[at], sems.at[chunk, k])
            for k, (weight, stage) in enumerate(zip(weights, stages))
        ]

    for chunk in range(chunks):
        for fetch in fetches(chunk):
            fetch.start()
    for chunk in range(chunks):
        for fetch in fetches(chunk):
            fetch.wait()
        at = slice(chunk * step, (chunk + 1) * step)
        for stage, acc in zip(stages, accs):
            product = jnp.dot(rows_ref[:, at], stage[at], preferred_element_type=jnp.float32)
            if chunk > 0:
                acc[...] += product
            else:
                acc[...] = product
    return [acc[...] for acc in accs]


def project_kernel(begin, carried, held, kind, fetch, after, *refs):
    refs = list(refs)
    target_ref = refs.pop(0) if kind == "routed" else None
    rows_ref = refs.pop(0)
    weights = [refs.pop(0), refs.pop(0)]
    given = [refs.pop(0), refs.pop(0)] if carried else None
    held_ref = refs.pop(0) if held else None
    refs = refs[after:]
    outs = [refs.pop(0), refs.pop(0)]
    if fetch:
        sums = fetched_product(rows_ref, weights, refs[:2], refs[2:4], refs[4])
    else:
        at = slice(begin, begin + rows_ref.shape[1])
        sums = [
            jnp.dot(rows_ref[...], weight[at], preferred_element_type=jnp.float32)
            for weight in weights
        ]
    if carried:
        sums = [ref[...] + product for ref, product in zip(given, sums)]
    if kind == "sums":
        for out, product in zip(outs, sums):
            out[...] = product
        return
    query, keyval = (product.astype(jnp.bfloat16) for product in sums)
    if kind == "routed":
        route(([held_ref[...]] if held else []) + [query], target_ref, outs[0])
    else:
        outs[0][...] = query
    outs[1][0] = keyval


def project(rows, weights, kind, begin=0, given=(), held=(), targets=(), slots=None, fetch=False, after=()):
    length, depth = rows.shape
    widths = [weight.shape[1] for weight in weights]
    columns = sum(widths)
    vmem = pl.BlockSpec(memory_space=pltpu.VMEM)
    if kind == "sums":
        shapes = [jax.ShapeDtypeStruct((length, width), jnp.float32) for width in widths]
    else:
        first = (*slots, widths[0]) if kind == "routed" else (length, widths[0])
        shapes = [
            jax.ShapeDtypeStruct(shape, jnp.bfloat16) for shape in (first, (1, length, widths[1]))
        ]
    scratch = []
    if fetch:
        scratch = [pltpu.VMEM((depth, width), jnp.bfloat16) for width in widths]
        scratch += [pltpu.VMEM((length, width), jnp.float32) for width in widths]
        scratch += [pltpu.SemaphoreType.DMA((math.gcd(depth // 256, 8), 2))]
    weight_spec = pl.BlockSpec(memory_space=pl.ANY) if fetch else vmem
    return pl.pallas_call(
        functools.partial(project_kernel, begin, bool(given), bool(held), kind, fetch, len(after)),
        out_shape=shapes,
        in_specs=[pl.BlockSpec(memory_space=pltpu.SMEM)] * len(targets)
        + [vmem, weight_spec, weight_spec]
        + [vmem] * (len(given) + len(held))
        + [pl.BlockSpec(memory_space=pl.ANY)] * len(after),
        out_specs=[vmem] * len(shapes),
        scratch_shapes=scratch,
        compiler_params=pltpu.CompilerParams(vmem_limit_bytes=(52 if fetch else 28) << 20),
        cost_estimate=pl.CostEstimate(
            flops=2 * length * depth * columns,
            bytes_accessed=2 * (length * depth + depth * columns + length * columns),
            transcendentals=0,
        ),
    )(*targets, rows, *weights, *given, *held, *after)


def touch_kernel(*refs):
    ref, out_ref = refs[0], refs[-1]
    out_ref[...] = ref[: out_ref.shape[0], : out_ref.shape[1]]


def touch(weights, *after):
    vmem = pl.BlockSpec(memory_space=pltpu.VMEM)
    hbm = pl.BlockSpec(memory_space=pl.ANY)
    return pl.pallas_call(
        touch_kernel,
        out_shape=jax.ShapeDtypeStruct((16, 128), weights[0].dtype),
        in_specs=[vmem] * len(weights) + [hbm] * len(after),
        out_specs=vmem,
        compiler_params=pltpu.CompilerParams(vmem_limit_bytes=20 << 20),
        name="touch",
    )(*weights, *after)


def gather_bits(count):
    bits = [1 << b for b in reversed(range(count.bit_length() - 1))]
    return bits[:1] + bits[2:3] + bits[1:2] + bits[3:]


def gather_all(part, count):
    pieces = [part]
    for bit in gather_bits(count):
        pairs = [(i, i ^ bit) for i in range(count)]
        held = pieces[0] if len(pieces) == 1 else jnp.concatenate(pieces, axis=0)
        pieces.append(lax.ppermute(held, "ctx", pairs))
    return pieces


def slots_of(refs):
    return [(ref, index) for ref in refs for index in range(ref.shape[0])]


def slot_source(slot, me, count):
    code = 0
    for place, bit in enumerate(gather_bits(count)):
        if slot >> place & 1:
            code |= bit
    return me ^ code


def attend_kernel(
    count,
    heads,
    segments,
    info_ref,
    source_ref,
    rank_ref,
    item_block_ref,
    item_tile_ref,
    start_ref,
    place_ref,
    arrived_refs,
    keyval_refs,
    out_ref,
    key_ref,
    value_ref,
    valt_ref,
    query_ref,
    max_ref,
    sum_ref,
    acc_ref,
):
    blocks, per_block = start_ref.shape
    block_len = arrived_refs[0].shape[1]
    dim = key_ref.shape[2]
    rows = key_ref.shape[1]
    me = info_ref[0]
    iterations = info_ref[1]
    own_place = info_ref[2]
    own_blocks = keyval_refs[0][0].shape[1] // block_len

    def place_rows(slots, piece_of, offset_at, first, length):
        row = pl.multiple_of(info_ref[offset_at] + first, 16)
        for slot in range(count):
            source = slot_source(slot, me, count)
            piece = piece_of(*slots[slot])
            key_ref[source, pl.ds(row, length), :] = piece[:, :dim]
            value_ref[source, pl.ds(row, length), :] = piece[:, dim:]

    for index, begin, offset_at, first, length in segments:
        place_rows(
            slots_of(keyval_refs[index]),
            lambda ref, slot: ref[slot, begin : begin + length, :],
            offset_at,
            first,
            length,
        )
    for tile in range(count):
        valt_ref[tile] = value_ref[tile].T

    for block in range(blocks):
        own = (block >= own_place) & (block < own_place + own_blocks)

        def take(ref, index):
            for head in range(heads):
                query_ref[block, head * block_len : (head + 1) * block_len, :] = ref[
                    index, :, head * dim : (head + 1) * dim
                ]

        @pl.when(own)
        def _():
            take(arrived_refs[0], source_ref[block])

        @pl.when(jnp.logical_not(own))
        def _():
            take(arrived_refs[1], source_ref[block])

    max_ref[...] = jnp.full_like(max_ref, NEG_FILL)
    sum_ref[...] = jnp.zeros_like(sum_ref)
    acc_ref[...] = jnp.zeros_like(acc_ref)
    key_index = lax.broadcasted_iota(jnp.int32, (rows, per_block), 0)
    scale = LOG2E / math.sqrt(dim)

    def step(iteration, carry):
        done = []
        for u in range(UNROLL):
            item = iteration * UNROLL + u
            block = item_block_ref[item]
            tile = item_tile_ref[item]
            safe = jnp.minimum(block, blocks - 1)
            scores = lax.dot_general(
                key_ref[tile],
                query_ref[safe],
                (((1,), (1,)), ((), ())),
                preferred_element_type=jnp.float32,
            )
            base = tile * rows
            start = start_ref[pl.ds(safe, 1), :] - base
            place = place_ref[pl.ds(safe, 1), :] - base
            allowed = (key_index >= start) & (key_index <= place)
            scores = jnp.where(allowed, scores * scale, NEG_FILL)
            highest = jnp.max(scores, axis=0, keepdims=True)
            weights = jnp.exp2(scores - highest)
            total = jnp.sum(weights, axis=0, keepdims=True)
            summed = lax.dot_general(
                valt_ref[tile],
                weights.astype(jnp.bfloat16),
                (((1,), (0,)), ((), ())),
                preferred_element_type=jnp.float32,
            )
            done.append((block, highest, total, summed))
        for block, highest, total, summed in done:
            old = max_ref[pl.ds(block, 1), :]
            new = jnp.maximum(old, highest)
            keep = jnp.exp2(old - new)
            add = jnp.exp2(highest - new)
            max_ref[pl.ds(block, 1), :] = new
            sum_ref[pl.ds(block, 1), :] = sum_ref[pl.ds(block, 1), :] * keep + total * add
            acc_ref[block] = acc_ref[block] * keep + summed * add
        return carry

    lax.fori_loop(0, iterations, step, 0)

    for block in range(blocks):
        result = (acc_ref[block] / sum_ref[block : block + 1, :]).T.astype(jnp.bfloat16)
        row = pl.multiple_of(rank_ref[block] * block_len, block_len)
        for head in range(heads):
            out_ref[pl.ds(row, block_len), head * dim : (head + 1) * dim] = result[
                head * block_len : (head + 1) * block_len, :
            ]


def step(tokens, query_weight, keyval_weight, doc_lengths, owners):
    count = lax.axis_size("ctx")
    me = lax.axis_index("ctx")
    groups = lax.axis_size("tp")
    member = lax.axis_index("tp")
    share, depth = tokens.shape
    rows = share * groups
    per = owners.shape[0] // count
    block_len = rows // per
    dim = keyval_weight.shape[1] // 2
    query_cols = query_weight.shape[1]
    heads = query_cols // dim
    share_blocks = share // block_len
    late = block_len * max(1, share_blocks // 2)
    rest = depth // 4

    pieces = [(shift, 0, share) for shift in range(1, groups - 1)]
    pieces += [(groups - 1, 0, share - late), (groups - 1, share - late, late)]
    head = min(16, pieces[0][2] // 2)

    def shifted(part, shift):
        return lax.ppermute(part, "tp", [(i, (i + shift) % groups) for i in range(groups)])

    grid = owners.reshape(count, per)
    place_of = jnp.arange(per, dtype=jnp.int32)
    sources = jnp.sum(
        jnp.where(grid == me, jnp.arange(count, dtype=jnp.int32)[:, None], 0), axis=0
    )
    mine = sources * per + place_of
    rank = jnp.sum((mine[None, :] < mine[:, None]).astype(jnp.int32), axis=1)
    length_count = doc_lengths.shape[0]
    order = jnp.arange(length_count)
    doc_ends = jnp.sum(
        jnp.where(order[None, :] <= order[:, None], doc_lengths[None, :], 0), axis=1
    )
    row_place = mine[:, None] * block_len + jnp.arange(block_len, dtype=jnp.int32)[None, :]
    row_start = jnp.max(
        jnp.where(doc_ends[None, None, :] <= row_place[:, :, None], doc_ends, 0), axis=2
    )
    first_tile = row_start[:, 0] // rows
    last_tile = row_place[:, -1] // rows
    tiles = last_tile - first_tile + 1
    before = jnp.sum(
        jnp.where(place_of[None, :] < place_of[:, None], tiles[None, :], 0), axis=1
    )
    item = jnp.arange(per * count + UNROLL, dtype=jnp.int32)
    within = (item[:, None] >= before[None, :]) & (item[:, None] < (before + tiles)[None, :])
    item_block = per - jnp.sum(jnp.where(within, per - place_of[None, :], 0), axis=1)
    item_tile = jnp.sum(
        jnp.where(within, first_tile[None, :] + item[:, None] - before[None, :], 0), axis=1
    )
    iterations = (jnp.sum(tiles) + UNROLL - 1) // UNROLL

    own_targets = lax.dynamic_index_in_dim(grid, me, 0, keepdims=False)

    def targets_of(shift, first, length):
        begin = ((member - shift) % groups) * share_blocks + first // block_len
        return lax.dynamic_slice_in_dim(own_targets, begin, length // block_len, 0)

    weights = (query_weight, keyval_weight)
    slots = (count, block_len)
    shift, first, length = pieces[0]
    early = [shifted(tokens[first : first + head], shift)]
    early.append(shifted(tokens[first + head : first + length], shift))
    for shift, first, length in pieces[1:-1]:
        early.append(shifted(tokens[first : first + length], shift))
    send_own, own_keyval = project(
        tokens, weights, "routed", targets=(targets_of(0, 0, share),), slots=slots, fetch=True
    )
    shift, first, length = pieces[-1]
    late_most = shifted(tokens[first : first + length, : depth - rest], shift)
    late_rest = shifted(tokens[first : first + length, depth - rest :], shift)
    gathered_own = gather_all(own_keyval, count)
    send_own, gathered_own[1] = lax.optimization_barrier((send_own, gathered_own[1]))
    arrived_own = lax.all_to_all(send_own, "ctx", 0, 0, tiled=True)
    early_rows = jnp.concatenate(early, axis=0)
    other_targets = jnp.concatenate([targets_of(*piece) for piece in pieces])
    touched = touch(weights, gathered_own[1], other_targets)
    early_query, early_keyval = project(early_rows, weights, "plain", after=(touched,))
    gathered_early = gather_all(early_keyval, count)
    sums = project(late_most, weights, "sums")
    send_other, late_keyval = project(
        late_rest,
        weights,
        "routed",
        begin=depth - rest,
        given=sums,
        held=(early_query,),
        targets=(other_targets,),
        slots=slots,
    )
    gathered_late = gather_all(late_keyval, count)
    arrived_other = lax.all_to_all(send_other, "ctx", 0, 0, tiled=True)

    segments = [(0, 0, 3, 0, share)]
    begin = 0
    for shift, first, length in pieces[:-1]:
        segments.append((1, begin, 3 + shift, first, length))
        begin += length
    segments.append((2, 0, 3 + pieces[-1][0], pieces[-1][1], late))
    offsets = [((member - shift) % groups) * share for shift in range(groups)]

    info = jnp.stack([me, iterations, member * share_blocks, *offsets]).astype(jnp.int32)
    per_block = heads * block_len
    smem = pl.BlockSpec(memory_space=pltpu.SMEM)
    vmem = pl.BlockSpec(memory_space=pltpu.VMEM)
    return pl.pallas_call(
        functools.partial(attend_kernel, count, heads, tuple(segments)),
        out_shape=jax.ShapeDtypeStruct((rows, query_cols), jnp.bfloat16),
        in_specs=[smem] * 5 + [vmem] * 2 + [[vmem] * 2, [[vmem] * len(gathered_late)] * 3],
        out_specs=vmem,
        scratch_shapes=[
            pltpu.VMEM((count, rows, dim), jnp.bfloat16),
            pltpu.VMEM((count, rows, dim), jnp.bfloat16),
            pltpu.VMEM((count, dim, rows), jnp.bfloat16),
            pltpu.VMEM((per, per_block, dim), jnp.bfloat16),
            pltpu.VMEM((per + 1, per_block), jnp.float32),
            pltpu.VMEM((per + 1, per_block), jnp.float32),
            pltpu.VMEM((per + 1, dim, per_block), jnp.float32),
        ],
        compiler_params=pltpu.CompilerParams(vmem_limit_bytes=16 << 20),
        name="attend",
    )(
        info,
        sources,
        rank,
        item_block,
        item_tile,
        jnp.tile(row_start, (1, heads)),
        jnp.tile(row_place, (1, heads)),
        [arrived_own, arrived_other],
        [gathered_own, gathered_early, gathered_late],
    )


def solution(mesh):
    return jax.shard_map(
        step,
        mesh=mesh,
        in_specs=(P(("ctx", "tp"), None), P(None, "tp"), P(None, "tp"), P(), P()),
        out_specs=P("ctx", "tp"),
        check_vma=False,
    )
```

```python
import functools
import math

import jax
import jax.numpy as jnp
from jax import lax
from jax.experimental import pallas as pl
from jax.experimental.pallas import tpu as pltpu
from jax.sharding import PartitionSpec as P


NEG_FILL = -1e30
LOG2E = 1.4426950408889634
UNROLL = 8


def route(queries, target_ref, send_ref):
    block_len = send_ref.shape[1]
    row = 0
    for query in queries:
        first = 0
        while first < query.shape[0]:
            block, at = divmod(row, block_len)
            length = min(block_len - at, query.shape[0] - first)
            send_ref[target_ref[block], at : at + length] = query[first : first + length]
            first, row = first + length, row + length


def fetched_product(rows_ref, weights, stages, accs, sems):
    chunks = sems.shape[0]
    step = rows_ref.shape[1] // chunks

    def fetches(chunk):
        at = pl.ds(chunk * step, step)
        return [
            pltpu.make_async_copy(weight.at[at], stage.at[at], sems.at[chunk, k])
            for k, (weight, stage) in enumerate(zip(weights, stages))
        ]

    for chunk in range(chunks):
        for fetch in fetches(chunk):
            fetch.start()
    for chunk in range(chunks):
        for fetch in fetches(chunk):
            fetch.wait()
        at = slice(chunk * step, (chunk + 1) * step)
        for stage, acc in zip(stages, accs):
            product = jnp.dot(rows_ref[:, at], stage[at], preferred_element_type=jnp.float32)
            if chunk > 0:
                acc[...] += product
            else:
                acc[...] = product
    return [acc[...] for acc in accs]


def project_kernel(parts, begin, carried, held, kind, fetch, after, *refs):
    refs = list(refs)
    target_ref = refs.pop(0) if kind == "routed" else None
    row_refs = [refs.pop(0) for _ in range(parts)]
    weights = [refs.pop(0), refs.pop(0)]
    given = [refs.pop(0), refs.pop(0)] if carried else None
    held_ref = refs.pop(0) if held else None
    refs = refs[after:]
    outs = [refs.pop(0), refs.pop(0)]
    if fetch:
        sums = fetched_product(row_refs[0], weights, refs[:2], refs[2:4], refs[4])
    else:
        rows = jnp.concatenate([ref[...] for ref in row_refs], axis=0)
        at = slice(begin, begin + rows.shape[1])
        sums = [
            jnp.dot(rows, weight[at], preferred_element_type=jnp.float32)
            for weight in weights
        ]
    if carried:
        sums = [ref[...] + product for ref, product in zip(given, sums)]
    if kind == "sums":
        for out, product in zip(outs, sums):
            out[...] = product
        return
    query, keyval = (product.astype(jnp.bfloat16) for product in sums)
    if kind == "routed":
        route(([held_ref[...]] if held else []) + [query], target_ref, outs[0])
    else:
        outs[0][...] = query
    outs[1][0] = keyval


def project(row_parts, weights, kind, begin=0, given=(), held=(), targets=(), slots=None, fetch=False, after=()):
    length, depth = sum(rows.shape[0] for rows in row_parts), row_parts[0].shape[1]
    widths = [weight.shape[1] for weight in weights]
    columns = sum(widths)
    vmem = pl.BlockSpec(memory_space=pltpu.VMEM)
    if kind == "sums":
        shapes = [jax.ShapeDtypeStruct((length, width), jnp.float32) for width in widths]
    else:
        first = (*slots, widths[0]) if kind == "routed" else (length, widths[0])
        shapes = [
            jax.ShapeDtypeStruct(shape, jnp.bfloat16) for shape in (first, (1, length, widths[1]))
        ]
    scratch = []
    if fetch:
        scratch = [pltpu.VMEM((depth, width), jnp.bfloat16) for width in widths]
        scratch += [pltpu.VMEM((length, width), jnp.float32) for width in widths]
        scratch += [pltpu.SemaphoreType.DMA((math.gcd(depth // 256, 8), 2))]
    weight_spec = pl.BlockSpec(memory_space=pl.ANY) if fetch else vmem
    return pl.pallas_call(
        functools.partial(
            project_kernel, len(row_parts), begin, bool(given), bool(held), kind, fetch, len(after)
        ),
        out_shape=shapes,
        in_specs=[pl.BlockSpec(memory_space=pltpu.SMEM)] * len(targets)
        + [vmem] * len(row_parts)
        + [weight_spec] * 2
        + [vmem] * (len(given) + len(held))
        + [pl.BlockSpec(memory_space=pl.ANY)] * len(after),
        out_specs=[vmem] * len(shapes),
        scratch_shapes=scratch,
        compiler_params=pltpu.CompilerParams(vmem_limit_bytes=(52 if fetch else 28) << 20),
        cost_estimate=pl.CostEstimate(
            flops=2 * length * depth * columns,
            bytes_accessed=2 * (length * depth + depth * columns + length * columns),
            transcendentals=0,
        ),
    )(*targets, *row_parts, *weights, *given, *held, *after)


def touch_kernel(*refs):
    ref, out_ref = refs[0], refs[-1]
    out_ref[...] = ref[: out_ref.shape[0], : out_ref.shape[1]]


def touch(weights, *after):
    vmem = pl.BlockSpec(memory_space=pltpu.VMEM)
    hbm = pl.BlockSpec(memory_space=pl.ANY)
    return pl.pallas_call(
        touch_kernel,
        out_shape=jax.ShapeDtypeStruct((16, 128), weights[0].dtype),
        in_specs=[vmem] * len(weights) + [hbm] * len(after),
        out_specs=vmem,
        compiler_params=pltpu.CompilerParams(vmem_limit_bytes=28 << 20),
        cost_estimate=pl.CostEstimate(
            flops=32 * weights[0].size, bytes_accessed=2 * weights[0].size, transcendentals=0
        ),
        name="touch",
    )(*weights, *after)


def gather_bits(count):
    bits = [1 << b for b in reversed(range(count.bit_length() - 1))]
    return bits[:1] + bits[2:3] + bits[1:2] + bits[3:]


def gather_all(part, count):
    pieces = [part]
    for bit in gather_bits(count):
        pairs = [(i, i ^ bit) for i in range(count)]
        held = pieces[0] if len(pieces) == 1 else jnp.concatenate(pieces, axis=0)
        pieces.append(lax.ppermute(held, "ctx", pairs))
    return pieces


def slots_of(refs):
    return [(ref, index) for ref in refs for index in range(ref.shape[0])]


def slot_source(slot, me, count):
    code = 0
    for place, bit in enumerate(gather_bits(count)):
        if slot >> place & 1:
            code |= bit
    return me ^ code


def attend_kernel(
    count,
    heads,
    segments,
    info_ref,
    source_ref,
    rank_ref,
    item_block_ref,
    item_tile_ref,
    start_ref,
    place_ref,
    arrived_refs,
    keyval_refs,
    out_ref,
    key_ref,
    value_ref,
    valt_ref,
    query_ref,
    max_ref,
    sum_ref,
    acc_ref,
):
    blocks, per_block = start_ref.shape
    block_len = arrived_refs[0].shape[1]
    dim = key_ref.shape[2]
    rows = key_ref.shape[1]
    me = info_ref[0]
    iterations = info_ref[1]
    own_place = info_ref[2]
    own_blocks = keyval_refs[0][0].shape[1] // block_len

    def place_rows(slots, piece_of, offset_at, first, length):
        row = pl.multiple_of(info_ref[offset_at] + first, 16)
        for slot in range(count):
            source = slot_source(slot, me, count)
            piece = piece_of(*slots[slot])
            key_ref[source, pl.ds(row, length), :] = piece[:, :dim]
            value_ref[source, pl.ds(row, length), :] = piece[:, dim:]

    for index, begin, offset_at, first, length in segments:
        place_rows(
            slots_of(keyval_refs[index]),
            lambda ref, slot: ref[slot, begin : begin + length, :],
            offset_at,
            first,
            length,
        )
    for tile in range(count):
        valt_ref[tile] = value_ref[tile].T

    for block in range(blocks):
        own = (block >= own_place) & (block < own_place + own_blocks)

        def take(ref, index):
            for head in range(heads):
                query_ref[block, head * block_len : (head + 1) * block_len, :] = ref[
                    index, :, head * dim : (head + 1) * dim
                ]

        @pl.when(own)
        def _():
            take(arrived_refs[0], source_ref[block])

        @pl.when(jnp.logical_not(own))
        def _():
            take(arrived_refs[1], source_ref[block])

    max_ref[...] = jnp.full_like(max_ref, NEG_FILL)
    sum_ref[...] = jnp.zeros_like(sum_ref)
    acc_ref[...] = jnp.zeros_like(acc_ref)
    key_index = lax.broadcasted_iota(jnp.int32, (rows, per_block), 0)
    scale = LOG2E / math.sqrt(dim)

    def step(iteration, carry):
        done = []
        for u in range(UNROLL):
            item = iteration * UNROLL + u
            block = item_block_ref[item]
            tile = item_tile_ref[item]
            safe = jnp.minimum(block, blocks - 1)
            scores = lax.dot_general(
                key_ref[tile],
                query_ref[safe],
                (((1,), (1,)), ((), ())),
                preferred_element_type=jnp.float32,
            )
            base = tile * rows
            start = start_ref[pl.ds(safe, 1), :] - base
            place = place_ref[pl.ds(safe, 1), :] - base
            allowed = (key_index >= start) & (key_index <= place)
            scores = jnp.where(allowed, scores * scale, NEG_FILL)
            highest = jnp.max(scores, axis=0, keepdims=True)
            weights = jnp.exp2(scores - highest)
            total = jnp.sum(weights, axis=0, keepdims=True)
            summed = lax.dot_general(
                valt_ref[tile],
                weights.astype(jnp.bfloat16),
                (((1,), (0,)), ((), ())),
                preferred_element_type=jnp.float32,
            )
            done.append((block, highest, total, summed))
        for block, highest, total, summed in done:
            old = max_ref[pl.ds(block, 1), :]
            new = jnp.maximum(old, highest)
            keep = jnp.exp2(old - new)
            add = jnp.exp2(highest - new)
            max_ref[pl.ds(block, 1), :] = new
            sum_ref[pl.ds(block, 1), :] = sum_ref[pl.ds(block, 1), :] * keep + total * add
            acc_ref[block] = acc_ref[block] * keep + summed * add
        return carry

    lax.fori_loop(0, iterations, step, 0)

    for block in range(blocks):
        result = (acc_ref[block] / sum_ref[block : block + 1, :]).T.astype(jnp.bfloat16)
        row = pl.multiple_of(rank_ref[block] * block_len, block_len)
        for head in range(heads):
            out_ref[pl.ds(row, block_len), head * dim : (head + 1) * dim] = result[
                head * block_len : (head + 1) * block_len, :
            ]


def step(tokens, query_weight, keyval_weight, doc_lengths, owners):
    count = lax.axis_size("ctx")
    me = lax.axis_index("ctx")
    groups = lax.axis_size("tp")
    member = lax.axis_index("tp")
    share, depth = tokens.shape
    rows = share * groups
    per = owners.shape[0] // count
    block_len = rows // per
    dim = keyval_weight.shape[1] // 2
    query_cols = query_weight.shape[1]
    heads = query_cols // dim
    share_blocks = share // block_len
    late = max(16, share * 3 // 8 // 16 * 16)
    rest = depth // 4

    pieces = [(shift, 0, share) for shift in range(1, groups - 1)]
    pieces += [(groups - 1, 0, share - late), (groups - 1, share - late, late)]
    head = min(16, pieces[0][2] // 2)

    def shifted(part, shift):
        return lax.ppermute(part, "tp", [(i, (i + shift) % groups) for i in range(groups)])

    grid = owners.reshape(count, per)
    place_of = jnp.arange(per, dtype=jnp.int32)
    sources = jnp.sum(
        jnp.where(grid == me, jnp.arange(count, dtype=jnp.int32)[:, None], 0), axis=0
    )
    mine = sources * per + place_of
    rank = jnp.sum((mine[None, :] < mine[:, None]).astype(jnp.int32), axis=1)
    length_count = doc_lengths.shape[0]
    order = jnp.arange(length_count)
    doc_ends = jnp.sum(
        jnp.where(order[None, :] <= order[:, None], doc_lengths[None, :], 0), axis=1
    )
    row_place = mine[:, None] * block_len + jnp.arange(block_len, dtype=jnp.int32)[None, :]
    row_start = jnp.max(
        jnp.where(doc_ends[None, None, :] <= row_place[:, :, None], doc_ends, 0), axis=2
    )
    first_tile = row_start[:, 0] // rows
    last_tile = row_place[:, -1] // rows
    tiles = last_tile - first_tile + 1
    before = jnp.sum(
        jnp.where(place_of[None, :] < place_of[:, None], tiles[None, :], 0), axis=1
    )
    item = jnp.arange(per * count + UNROLL, dtype=jnp.int32)
    within = (item[:, None] >= before[None, :]) & (item[:, None] < (before + tiles)[None, :])
    item_block = per - jnp.sum(jnp.where(within, per - place_of[None, :], 0), axis=1)
    item_tile = jnp.sum(
        jnp.where(within, first_tile[None, :] + item[:, None] - before[None, :], 0), axis=1
    )
    iterations = (jnp.sum(tiles) + UNROLL - 1) // UNROLL

    own_targets = lax.dynamic_index_in_dim(grid, me, 0, keepdims=False)

    def targets_of(shift):
        begin = ((member - shift) % groups) * share_blocks
        return lax.dynamic_slice_in_dim(own_targets, begin, share_blocks, 0)

    weights = (query_weight, keyval_weight)
    slots = (count, block_len)
    shift, first, length = pieces[0]
    early = [shifted(tokens[first : first + head], shift)]
    early.append(shifted(tokens[first + head : first + length], shift))
    for shift, first, length in pieces[1:-1]:
        early.append(shifted(tokens[first : first + length], shift))
    send_own, own_keyval = project(
        [tokens], weights, "routed", targets=(targets_of(0),), slots=slots, fetch=True
    )
    shift, first, length = pieces[-1]
    late_most = shifted(tokens[first : first + length, : depth - rest], shift)
    late_rest = shifted(tokens[first : first + length, depth - rest :], shift)
    gathered_own = gather_all(own_keyval, count)
    send_own, gathered_own[1] = lax.optimization_barrier((send_own, gathered_own[1]))
    arrived_own = lax.all_to_all(send_own, "ctx", 0, 0, tiled=True)
    other_targets = jnp.concatenate([targets_of(shift) for shift in range(1, groups)])
    touched = touch(weights, gathered_own[1], other_targets)
    early_query, early_keyval = project(early, weights, "plain", after=(touched,))
    gathered_early = gather_all(early_keyval, count)
    sums = project([late_most], weights, "sums")
    send_other, late_keyval = project(
        [late_rest],
        weights,
        "routed",
        begin=depth - rest,
        given=sums,
        held=(early_query,),
        targets=(other_targets,),
        slots=slots,
    )
    gathered_late = gather_all(late_keyval, count)
    arrived_other = lax.all_to_all(send_other, "ctx", 0, 0, tiled=True)

    segments = [(0, 0, 3, 0, share)]
    begin = 0
    for shift, first, length in pieces[:-1]:
        segments.append((1, begin, 3 + shift, first, length))
        begin += length
    segments.append((2, 0, 3 + pieces[-1][0], pieces[-1][1], late))
    offsets = [((member - shift) % groups) * share for shift in range(groups)]

    info = jnp.stack([me, iterations, member * share_blocks, *offsets]).astype(jnp.int32)
    per_block = heads * block_len
    smem = pl.BlockSpec(memory_space=pltpu.SMEM)
    vmem = pl.BlockSpec(memory_space=pltpu.VMEM)
    return pl.pallas_call(
        functools.partial(attend_kernel, count, heads, tuple(segments)),
        out_shape=jax.ShapeDtypeStruct((rows, query_cols), jnp.bfloat16),
        in_specs=[smem] * 5 + [vmem] * 2 + [[vmem] * 2, [[vmem] * len(gathered_late)] * 3],
        out_specs=vmem,
        scratch_shapes=[
            pltpu.VMEM((count, rows, dim), jnp.bfloat16),
            pltpu.VMEM((count, rows, dim), jnp.bfloat16),
            pltpu.VMEM((count, dim, rows), jnp.bfloat16),
            pltpu.VMEM((per, per_block, dim), jnp.bfloat16),
            pltpu.VMEM((per + 1, per_block), jnp.float32),
            pltpu.VMEM((per + 1, per_block), jnp.float32),
            pltpu.VMEM((per + 1, dim, per_block), jnp.float32),
        ],
        compiler_params=pltpu.CompilerParams(vmem_limit_bytes=16 << 20),
        name="attend",
    )(
        info,
        sources,
        rank,
        item_block,
        item_tile,
        jnp.tile(row_start, (1, heads)),
        jnp.tile(row_place, (1, heads)),
        [arrived_own, arrived_other],
        [gathered_own, gathered_early, gathered_late],
    )


def solution(mesh):
    return jax.shard_map(
        step,
        mesh=mesh,
        in_specs=(P(("ctx", "tp"), None), P(None, "tp"), P(None, "tp"), P(), P()),
        out_specs=P("ctx", "tp"),
        check_vma=False,
    )
```

```python
import functools
import math

import jax
import jax.numpy as jnp
from jax import lax
from jax.experimental import pallas as pl
from jax.experimental.pallas import tpu as pltpu
from jax.sharding import PartitionSpec as P


NEG_FILL = -1e30
LOG2E = 1.4426950408889634
UNROLL = 8


def route(queries, target_ref, send_ref):
    block_len = send_ref.shape[1]
    row = 0
    for query in queries:
        first = 0
        while first < query.shape[0]:
            block, at = divmod(row, block_len)
            length = min(block_len - at, query.shape[0] - first)
            send_ref[target_ref[block], at : at + length] = query[first : first + length]
            first, row = first + length, row + length


def project_kernel(parts, begin, carried, held, kind, after, *refs):
    refs = list(refs)
    target_ref = refs.pop(0) if kind == "routed" else None
    row_refs = [refs.pop(0) for _ in range(parts)]
    weights = [refs.pop(0), refs.pop(0)]
    given = [refs.pop(0), refs.pop(0)] if carried else None
    held_refs = [refs.pop(0) for _ in range(held)]
    refs = refs[after:]
    outs = [refs.pop(0), refs.pop(0)]
    rows = jnp.concatenate([ref[...] for ref in row_refs], axis=0)
    at = slice(begin, begin + rows.shape[1])
    sums = [
        jnp.dot(rows, weight[at], preferred_element_type=jnp.float32) for weight in weights
    ]
    if carried:
        sums = [ref[...] + product for ref, product in zip(given, sums)]
    if kind == "sums":
        for out, product in zip(outs, sums):
            out[...] = product
        return
    query, keyval = (product.astype(jnp.bfloat16) for product in sums)
    if kind == "routed":
        route([ref[...] for ref in held_refs] + [query], target_ref, outs[0])
    else:
        outs[0][...] = query
    outs[1][0] = keyval


def project(row_parts, weights, kind, begin=0, given=(), held=(), targets=(), slots=None, after=()):
    length, depth = sum(rows.shape[0] for rows in row_parts), row_parts[0].shape[1]
    widths = [weight.shape[1] for weight in weights]
    columns = sum(widths)
    vmem = pl.BlockSpec(memory_space=pltpu.VMEM)
    if kind == "sums":
        shapes = [jax.ShapeDtypeStruct((length, width), jnp.float32) for width in widths]
    else:
        first = (*slots, widths[0]) if kind == "routed" else (length, widths[0])
        shapes = [
            jax.ShapeDtypeStruct(shape, jnp.bfloat16) for shape in (first, (1, length, widths[1]))
        ]
    return pl.pallas_call(
        functools.partial(
            project_kernel, len(row_parts), begin, bool(given), len(held), kind, len(after)
        ),
        out_shape=shapes,
        in_specs=[pl.BlockSpec(memory_space=pltpu.SMEM)] * len(targets)
        + [vmem] * len(row_parts)
        + [vmem] * 2
        + [vmem] * (len(given) + len(held))
        + [pl.BlockSpec(memory_space=pl.ANY)] * len(after),
        out_specs=[vmem] * len(shapes),
        compiler_params=pltpu.CompilerParams(vmem_limit_bytes=28 << 20),
        cost_estimate=pl.CostEstimate(
            flops=2 * length * depth * columns,
            bytes_accessed=2 * (length * depth + depth * columns + length * columns),
            transcendentals=0,
        ),
    )(*targets, *row_parts, *weights, *given, *held, *after)


def gather_bits(count):
    bits = [1 << b for b in reversed(range(count.bit_length() - 1))]
    return bits[:1] + bits[2:3] + bits[1:2] + bits[3:]


def gather_all(part, count):
    pieces = [part]
    for bit in gather_bits(count):
        pairs = [(i, i ^ bit) for i in range(count)]
        held = pieces[0] if len(pieces) == 1 else jnp.concatenate(pieces, axis=0)
        pieces.append(lax.ppermute(held, "ctx", pairs))
    return pieces


def slots_of(refs):
    return [(ref, index) for ref in refs for index in range(ref.shape[0])]


def slot_source(slot, me, count):
    code = 0
    for place, bit in enumerate(gather_bits(count)):
        if slot >> place & 1:
            code |= bit
    return me ^ code


def attend_kernel(
    count,
    heads,
    segments,
    info_ref,
    source_ref,
    rank_ref,
    item_block_ref,
    item_tile_ref,
    start_ref,
    place_ref,
    arrived_ref,
    keyval_refs,
    out_ref,
    key_ref,
    value_ref,
    valt_ref,
    query_ref,
    max_ref,
    sum_ref,
    acc_ref,
):
    blocks, per_block = start_ref.shape
    block_len = arrived_ref.shape[1]
    dim = key_ref.shape[2]
    rows = key_ref.shape[1]
    me = info_ref[0]
    iterations = info_ref[1]

    def place_rows(slots, piece_of, offset_at, first, length):
        row = pl.multiple_of(info_ref[offset_at] + first, 16)
        for slot in range(count):
            source = slot_source(slot, me, count)
            piece = piece_of(*slots[slot])
            key_ref[source, pl.ds(row, length), :] = piece[:, :dim]
            value_ref[source, pl.ds(row, length), :] = piece[:, dim:]

    for index, begin, offset_at, first, length in segments:
        place_rows(
            slots_of(keyval_refs[index]),
            lambda ref, slot: ref[slot, begin : begin + length, :],
            offset_at,
            first,
            length,
        )
    for tile in range(count):
        valt_ref[tile] = value_ref[tile].T

    for block in range(blocks):
        for head in range(heads):
            query_ref[block, head * block_len : (head + 1) * block_len, :] = arrived_ref[
                source_ref[block], :, head * dim : (head + 1) * dim
            ]

    max_ref[...] = jnp.full_like(max_ref, NEG_FILL)
    sum_ref[...] = jnp.zeros_like(sum_ref)
    acc_ref[...] = jnp.zeros_like(acc_ref)
    key_index = lax.broadcasted_iota(jnp.int32, (rows, per_block), 0)
    scale = LOG2E / math.sqrt(dim)

    def step(iteration, carry):
        done = []
        for u in range(UNROLL):
            item = iteration * UNROLL + u
            block = item_block_ref[item]
            tile = item_tile_ref[item]
            safe = jnp.minimum(block, blocks - 1)
            scores = lax.dot_general(
                key_ref[tile],
                query_ref[safe],
                (((1,), (1,)), ((), ())),
                preferred_element_type=jnp.float32,
            )
            base = tile * rows
            start = start_ref[pl.ds(safe, 1), :] - base
            place = place_ref[pl.ds(safe, 1), :] - base
            allowed = (key_index - start).astype(jnp.uint32) <= (place - start).astype(jnp.uint32)
            scores = jnp.where(allowed, scores * scale, NEG_FILL)
            highest = jnp.max(scores, axis=0, keepdims=True)
            weights = jnp.exp2(scores - highest)
            total = jnp.sum(weights, axis=0, keepdims=True)
            summed = lax.dot_general(
                valt_ref[tile],
                weights.astype(jnp.bfloat16),
                (((1,), (0,)), ((), ())),
                preferred_element_type=jnp.float32,
            )
            done.append((block, highest, total, summed))
        for block, highest, total, summed in done:
            old = max_ref[pl.ds(block, 1), :]
            new = jnp.maximum(old, highest)
            keep = jnp.exp2(old - new)
            add = jnp.exp2(highest - new)
            max_ref[pl.ds(block, 1), :] = new
            sum_ref[pl.ds(block, 1), :] = sum_ref[pl.ds(block, 1), :] * keep + total * add
            acc_ref[block] = acc_ref[block] * keep + summed * add
        return carry

    lax.fori_loop(0, iterations, step, 0)

    for block in range(blocks):
        result = (acc_ref[block] / sum_ref[block : block + 1, :]).T.astype(jnp.bfloat16)
        row = pl.multiple_of(rank_ref[block] * block_len, block_len)
        for head in range(heads):
            out_ref[pl.ds(row, block_len), head * dim : (head + 1) * dim] = result[
                head * block_len : (head + 1) * block_len, :
            ]


def step(tokens, query_weight, keyval_weight, doc_lengths, owners):
    count = lax.axis_size("ctx")
    me = lax.axis_index("ctx")
    groups = lax.axis_size("tp")
    member = lax.axis_index("tp")
    share, depth = tokens.shape
    rows = share * groups
    per = owners.shape[0] // count
    block_len = rows // per
    dim = keyval_weight.shape[1] // 2
    query_cols = query_weight.shape[1]
    heads = query_cols // dim
    share_blocks = share // block_len
    late = max(16, share * 3 // 8 // 16 * 16)
    rest = depth // 4

    pieces = [(shift, 0, share) for shift in range(1, groups - 1)]
    pieces += [(groups - 1, 0, share - late), (groups - 1, share - late, late)]
    head = min(16, pieces[0][2] // 2)

    def shifted(part, shift):
        return lax.ppermute(part, "tp", [(i, (i + shift) % groups) for i in range(groups)])

    grid = owners.reshape(count, per)
    place_of = jnp.arange(per, dtype=jnp.int32)
    sources = jnp.sum(
        jnp.where(grid == me, jnp.arange(count, dtype=jnp.int32)[:, None], 0), axis=0
    )
    mine = sources * per + place_of
    rank = jnp.sum((mine[None, :] < mine[:, None]).astype(jnp.int32), axis=1)
    length_count = doc_lengths.shape[0]
    order = jnp.arange(length_count)
    doc_ends = jnp.sum(
        jnp.where(order[None, :] <= order[:, None], doc_lengths[None, :], 0), axis=1
    )
    row_place = mine[:, None] * block_len + jnp.arange(block_len, dtype=jnp.int32)[None, :]
    row_start = jnp.max(
        jnp.where(doc_ends[None, None, :] <= row_place[:, :, None], doc_ends, 0), axis=2
    )
    first_tile = row_start[:, 0] // rows
    last_tile = row_place[:, -1] // rows
    tiles = last_tile - first_tile + 1
    before = jnp.sum(
        jnp.where(place_of[None, :] < place_of[:, None], tiles[None, :], 0), axis=1
    )
    item = jnp.arange(per * count + UNROLL, dtype=jnp.int32)
    within = (item[:, None] >= before[None, :]) & (item[:, None] < (before + tiles)[None, :])
    item_block = per - jnp.sum(jnp.where(within, per - place_of[None, :], 0), axis=1)
    item_tile = jnp.sum(
        jnp.where(within, first_tile[None, :] + item[:, None] - before[None, :], 0), axis=1
    )
    iterations = (jnp.sum(tiles) + UNROLL - 1) // UNROLL

    own_targets = lax.dynamic_index_in_dim(grid, me, 0, keepdims=False)

    def targets_of(shift):
        begin = ((member - shift) % groups) * share_blocks
        return lax.dynamic_slice_in_dim(own_targets, begin, share_blocks, 0)

    offsets = [((member - shift) % groups) * share for shift in range(groups)]
    info = jnp.stack([me, iterations, *offsets]).astype(jnp.int32)
    starts = jnp.tile(row_start, (1, heads))
    places = jnp.tile(row_place, (1, heads))
    targets = jnp.concatenate([targets_of(shift) for shift in range(groups)])
    integers = (info, sources, rank, item_block, item_tile, starts, places, targets)
    weights = (query_weight, keyval_weight)
    slots = (count, block_len)
    shift, first, length = pieces[0]
    early = [shifted(tokens[first : first + head], shift)]
    early.append(shifted(tokens[first + head : first + length], shift))
    for shift, first, length in pieces[1:-1]:
        early.append(shifted(tokens[first : first + length], shift))
    own_query, own_keyval = project([tokens], weights, "plain", after=integers)
    shift, first, length = pieces[-1]
    late_most = shifted(tokens[first : first + length, : depth - rest], shift)
    late_rest = shifted(tokens[first : first + length, depth - rest :], shift)
    gathered_own = gather_all(own_keyval, count)
    early_query, early_keyval = project(early, weights, "plain")
    gathered_early = gather_all(early_keyval, count)
    sums = project([late_most], weights, "sums")
    send, late_keyval = project(
        [late_rest],
        weights,
        "routed",
        begin=depth - rest,
        given=sums,
        held=(own_query, early_query),
        targets=(targets,),
        slots=slots,
    )
    gathered_late = gather_all(late_keyval, count)
    arrived = lax.all_to_all(send, "ctx", 0, 0, tiled=True)

    segments = [(0, 0, 2, 0, share)]
    begin = 0
    for shift, first, length in pieces[:-1]:
        segments.append((1, begin, 2 + shift, first, length))
        begin += length
    segments.append((2, 0, 2 + pieces[-1][0], pieces[-1][1], late))

    per_block = heads * block_len
    smem = pl.BlockSpec(memory_space=pltpu.SMEM)
    vmem = pl.BlockSpec(memory_space=pltpu.VMEM)
    return pl.pallas_call(
        functools.partial(attend_kernel, count, heads, tuple(segments)),
        out_shape=jax.ShapeDtypeStruct((rows, query_cols), jnp.bfloat16),
        in_specs=[smem] * 5 + [vmem] * 2 + [vmem, [[vmem] * len(gathered_late)] * 3],
        out_specs=vmem,
        scratch_shapes=[
            pltpu.VMEM((count, rows, dim), jnp.bfloat16),
            pltpu.VMEM((count, rows, dim), jnp.bfloat16),
            pltpu.VMEM((count, dim, rows), jnp.bfloat16),
            pltpu.VMEM((per, per_block, dim), jnp.bfloat16),
            pltpu.VMEM((per + 1, per_block), jnp.float32),
            pltpu.VMEM((per + 1, per_block), jnp.float32),
            pltpu.VMEM((per + 1, dim, per_block), jnp.float32),
        ],
        compiler_params=pltpu.CompilerParams(vmem_limit_bytes=16 << 20),
        name="attend",
    )(
        info,
        sources,
        rank,
        item_block,
        item_tile,
        starts,
        places,
        arrived,
        [gathered_own, gathered_early, gathered_late],
    )


def solution(mesh):
    return jax.shard_map(
        step,
        mesh=mesh,
        in_specs=(P(("ctx", "tp"), None), P(None, "tp"), P(None, "tp"), P(), P()),
        out_specs=P("ctx", "tp"),
        check_vma=False,
    )
```

```python
import functools
import math

import jax
import jax.numpy as jnp
from jax import lax
from jax.experimental import pallas as pl
from jax.experimental.pallas import tpu as pltpu
from jax.sharding import PartitionSpec as P


NEG_FILL = -1e30
LOG2E = 1.4426950408889634
UNROLL = 12


def route(queries, target_ref, send_ref):
    block_len = send_ref.shape[1]
    row = 0
    for query in queries:
        first = 0
        while first < query.shape[0]:
            block, at = divmod(row, block_len)
            length = min(block_len - at, query.shape[0] - first)
            send_ref[target_ref[block], at : at + length] = query[first : first + length]
            first, row = first + length, row + length


def project_kernel(parts, begin, carried, held, kind, after, *refs):
    refs = list(refs)
    target_ref = refs.pop(0) if kind == "routed" else None
    row_refs = [refs.pop(0) for _ in range(parts)]
    weights = [refs.pop(0), refs.pop(0)]
    given = [refs.pop(0), refs.pop(0)] if carried else None
    held_refs = [refs.pop(0) for _ in range(held)]
    refs = refs[after:]
    outs = [refs.pop(0), refs.pop(0)]
    rows = jnp.concatenate([ref[...] for ref in row_refs], axis=0)
    at = slice(begin, begin + rows.shape[1])
    sums = [
        jnp.dot(rows, weight[at], preferred_element_type=jnp.float32) for weight in weights
    ]
    if carried:
        sums = [ref[...] + product for ref, product in zip(given, sums)]
    if kind == "sums":
        for out, product in zip(outs, sums):
            out[...] = product
        return
    query, keyval = (product.astype(jnp.bfloat16) for product in sums)
    if kind == "routed":
        route([ref[...] for ref in held_refs] + [query], target_ref, outs[0])
    else:
        outs[0][...] = query
    outs[1][0] = keyval


def project(row_parts, weights, kind, begin=0, given=(), held=(), targets=(), slots=None, after=()):
    length, depth = sum(rows.shape[0] for rows in row_parts), row_parts[0].shape[1]
    widths = [weight.shape[1] for weight in weights]
    columns = sum(widths)
    vmem = pl.BlockSpec(memory_space=pltpu.VMEM)
    if kind == "sums":
        shapes = [jax.ShapeDtypeStruct((length, width), jnp.float32) for width in widths]
    else:
        first = (*slots, widths[0]) if kind == "routed" else (length, widths[0])
        shapes = [
            jax.ShapeDtypeStruct(shape, jnp.bfloat16) for shape in (first, (1, length, widths[1]))
        ]
    return pl.pallas_call(
        functools.partial(
            project_kernel, len(row_parts), begin, bool(given), len(held), kind, len(after)
        ),
        out_shape=shapes,
        in_specs=[pl.BlockSpec(memory_space=pltpu.SMEM)] * len(targets)
        + [vmem] * len(row_parts)
        + [vmem] * 2
        + [vmem] * (len(given) + len(held))
        + [pl.BlockSpec(memory_space=pl.ANY)] * len(after),
        out_specs=[vmem] * len(shapes),
        compiler_params=pltpu.CompilerParams(vmem_limit_bytes=28 << 20),
        cost_estimate=pl.CostEstimate(
            flops=2 * length * depth * columns,
            bytes_accessed=2 * (length * depth + depth * columns + length * columns),
            transcendentals=0,
        ),
    )(*targets, *row_parts, *weights, *given, *held, *after)


def gather_bits(count):
    bits = [1 << b for b in reversed(range(count.bit_length() - 1))]
    return bits[:1] + bits[2:3] + bits[1:2] + bits[3:]


def gather_all(part, count):
    pieces = [part]
    for bit in gather_bits(count):
        pairs = [(i, i ^ bit) for i in range(count)]
        held = pieces[0] if len(pieces) == 1 else jnp.concatenate(pieces, axis=0)
        pieces.append(lax.ppermute(held, "ctx", pairs))
    return pieces


def slots_of(refs):
    return [(ref, index) for ref in refs for index in range(ref.shape[0])]


def slot_source(slot, me, count):
    code = 0
    for place, bit in enumerate(gather_bits(count)):
        if slot >> place & 1:
            code |= bit
    return me ^ code


def attend_kernel(
    count,
    heads,
    segments,
    info_ref,
    source_ref,
    rank_ref,
    item_block_ref,
    item_tile_ref,
    start_ref,
    place_ref,
    arrived_ref,
    keyval_refs,
    out_ref,
    key_ref,
    value_ref,
    valt_ref,
    query_ref,
    max_ref,
    sum_ref,
    acc_ref,
):
    blocks, per_block = start_ref.shape
    block_len = arrived_ref.shape[1]
    dim = key_ref.shape[2]
    rows = key_ref.shape[1]
    me = info_ref[0]
    iterations = info_ref[1]

    def place_rows(slots, piece_of, offset_at, first, length):
        row = pl.multiple_of(info_ref[offset_at] + first, 16)
        for slot in range(count):
            source = slot_source(slot, me, count)
            piece = piece_of(*slots[slot])
            key_ref[source, pl.ds(row, length), :] = piece[:, :dim]
            value_ref[source, pl.ds(row, length), :] = piece[:, dim:]

    for index, begin, offset_at, first, length in segments:
        place_rows(
            slots_of(keyval_refs[index]),
            lambda ref, slot: ref[slot, begin : begin + length, :],
            offset_at,
            first,
            length,
        )
    for tile in range(count):
        valt_ref[tile] = value_ref[tile].T

    for block in range(blocks):
        heads_rows = [
            arrived_ref[source_ref[block], :, head * dim : (head + 1) * dim]
            for head in range(heads)
        ]
        query_ref[block] = jnp.concatenate(heads_rows, axis=0).T

    max_ref[...] = jnp.full_like(max_ref, NEG_FILL)
    sum_ref[...] = jnp.zeros_like(sum_ref)
    acc_ref[...] = jnp.zeros_like(acc_ref)
    key_index = lax.broadcasted_iota(jnp.int32, (rows, per_block), 0)
    scale = LOG2E / math.sqrt(dim)

    def step(iteration, carry):
        done = []
        for u in range(UNROLL):
            item = iteration * UNROLL + u
            block = item_block_ref[item]
            tile = item_tile_ref[item]
            safe = jnp.minimum(block, blocks - 1)
            scores = lax.dot_general(
                key_ref[tile],
                query_ref[safe],
                (((1,), (0,)), ((), ())),
                preferred_element_type=jnp.float32,
            )
            base = tile * rows
            start = start_ref[pl.ds(safe, 1), :] - base
            place = place_ref[pl.ds(safe, 1), :] - base
            allowed = (key_index - start).astype(jnp.uint32) <= (place - start).astype(jnp.uint32)
            scores = jnp.where(allowed, scores * scale, NEG_FILL)
            highest = jnp.max(scores, axis=0, keepdims=True)
            weights = jnp.exp2(scores - highest)
            total = jnp.sum(weights, axis=0, keepdims=True)
            summed = lax.dot_general(
                valt_ref[tile],
                weights.astype(jnp.bfloat16),
                (((1,), (0,)), ((), ())),
                preferred_element_type=jnp.float32,
            )
            done.append((block, highest, total, summed))
        for block, highest, total, summed in done:
            old = max_ref[pl.ds(block, 1), :]
            new = jnp.maximum(old, highest)
            keep = jnp.exp2(old - new)
            add = jnp.exp2(highest - new)
            max_ref[pl.ds(block, 1), :] = new
            sum_ref[pl.ds(block, 1), :] = sum_ref[pl.ds(block, 1), :] * keep + total * add
            acc_ref[block] = acc_ref[block] * keep + summed * add
        return carry

    lax.fori_loop(0, iterations, step, 0)

    for block in range(blocks):
        result = (acc_ref[block] / sum_ref[block : block + 1, :]).T.astype(jnp.bfloat16)
        row = pl.multiple_of(rank_ref[block] * block_len, block_len)
        for head in range(heads):
            out_ref[pl.ds(row, block_len), head * dim : (head + 1) * dim] = result[
                head * block_len : (head + 1) * block_len, :
            ]


def step(tokens, query_weight, keyval_weight, doc_lengths, owners):
    count = lax.axis_size("ctx")
    me = lax.axis_index("ctx")
    groups = lax.axis_size("tp")
    member = lax.axis_index("tp")
    share, depth = tokens.shape
    rows = share * groups
    per = owners.shape[0] // count
    block_len = rows // per
    dim = keyval_weight.shape[1] // 2
    query_cols = query_weight.shape[1]
    heads = query_cols // dim
    share_blocks = share // block_len
    late = max(16, share * 3 // 8 // 16 * 16)
    rest = depth // 4

    pieces = [(shift, 0, share) for shift in range(1, groups - 1)]
    pieces += [(groups - 1, 0, share - late), (groups - 1, share - late, late)]
    head = min(16, pieces[0][2] // 2)

    def shifted(part, shift):
        return lax.ppermute(part, "tp", [(i, (i + shift) % groups) for i in range(groups)])

    grid = owners.reshape(count, per)
    place_of = jnp.arange(per, dtype=jnp.int32)
    sources = jnp.sum(
        jnp.where(grid == me, jnp.arange(count, dtype=jnp.int32)[:, None], 0), axis=0
    )
    mine = sources * per + place_of
    rank = jnp.sum((mine[None, :] < mine[:, None]).astype(jnp.int32), axis=1)
    length_count = doc_lengths.shape[0]
    order = jnp.arange(length_count)
    doc_ends = jnp.sum(
        jnp.where(order[None, :] <= order[:, None], doc_lengths[None, :], 0), axis=1
    )
    row_place = mine[:, None] * block_len + jnp.arange(block_len, dtype=jnp.int32)[None, :]
    row_start = jnp.max(
        jnp.where(doc_ends[None, None, :] <= row_place[:, :, None], doc_ends, 0), axis=2
    )
    first_tile = row_start[:, 0] // rows
    last_tile = row_place[:, -1] // rows
    tiles = last_tile - first_tile + 1
    before = jnp.sum(
        jnp.where(place_of[None, :] < place_of[:, None], tiles[None, :], 0), axis=1
    )
    item = jnp.arange(per * count + UNROLL, dtype=jnp.int32)
    within = (item[:, None] >= before[None, :]) & (item[:, None] < (before + tiles)[None, :])
    item_block = per - jnp.sum(jnp.where(within, per - place_of[None, :], 0), axis=1)
    item_tile = jnp.sum(
        jnp.where(within, first_tile[None, :] + item[:, None] - before[None, :], 0), axis=1
    )
    iterations = (jnp.sum(tiles) + UNROLL - 1) // UNROLL

    own_targets = lax.dynamic_index_in_dim(grid, me, 0, keepdims=False)

    def targets_of(shift):
        begin = ((member - shift) % groups) * share_blocks
        return lax.dynamic_slice_in_dim(own_targets, begin, share_blocks, 0)

    offsets = [((member - shift) % groups) * share for shift in range(groups)]
    info = jnp.stack([me, iterations, *offsets]).astype(jnp.int32)
    starts = jnp.tile(row_start, (1, heads))
    places = jnp.tile(row_place, (1, heads))
    targets = jnp.concatenate([targets_of(shift) for shift in range(groups)])
    integers = (info, sources, rank, item_block, item_tile, starts, places, targets)
    weights = (query_weight, keyval_weight)
    slots = (count, block_len)
    shift, first, length = pieces[0]
    early = [shifted(tokens[first : first + head], shift)]
    early.append(shifted(tokens[first + head : first + length], shift))
    for shift, first, length in pieces[1:-1]:
        early.append(shifted(tokens[first : first + length], shift))
    own_query, own_keyval = project([tokens], weights, "plain", after=integers)
    shift, first, length = pieces[-1]
    late_most = shifted(tokens[first : first + length, : depth - rest], shift)
    late_rest = shifted(tokens[first : first + length, depth - rest :], shift)
    gathered_own = gather_all(own_keyval, count)
    early_query, early_keyval = project(early, weights, "plain")
    gathered_early = gather_all(early_keyval, count)
    sums = project([late_most], weights, "sums")
    send, late_keyval = project(
        [late_rest],
        weights,
        "routed",
        begin=depth - rest,
        given=sums,
        held=(own_query, early_query),
        targets=(targets,),
        slots=slots,
    )
    gathered_late = gather_all(late_keyval, count)
    arrived = lax.all_to_all(send, "ctx", 0, 0, tiled=True)

    segments = [(0, 0, 2, 0, share)]
    begin = 0
    for shift, first, length in pieces[:-1]:
        segments.append((1, begin, 2 + shift, first, length))
        begin += length
    segments.append((2, 0, 2 + pieces[-1][0], pieces[-1][1], late))

    per_block = heads * block_len
    smem = pl.BlockSpec(memory_space=pltpu.SMEM)
    vmem = pl.BlockSpec(memory_space=pltpu.VMEM)
    return pl.pallas_call(
        functools.partial(attend_kernel, count, heads, tuple(segments)),
        out_shape=jax.ShapeDtypeStruct((rows, query_cols), jnp.bfloat16),
        in_specs=[smem] * 5 + [vmem] * 2 + [vmem, [[vmem] * len(gathered_late)] * 3],
        out_specs=vmem,
        scratch_shapes=[
            pltpu.VMEM((count, rows, dim), jnp.bfloat16),
            pltpu.VMEM((count, rows, dim), jnp.bfloat16),
            pltpu.VMEM((count, dim, rows), jnp.bfloat16),
            pltpu.VMEM((per, dim, per_block), jnp.bfloat16),
            pltpu.VMEM((per + 1, per_block), jnp.float32),
            pltpu.VMEM((per + 1, per_block), jnp.float32),
            pltpu.VMEM((per + 1, dim, per_block), jnp.float32),
        ],
        compiler_params=pltpu.CompilerParams(vmem_limit_bytes=16 << 20),
        name="attend",
    )(
        info,
        sources,
        rank,
        item_block,
        item_tile,
        starts,
        places,
        arrived,
        [gathered_own, gathered_early, gathered_late],
    )


def solution(mesh):
    return jax.shard_map(
        step,
        mesh=mesh,
        in_specs=(P(("ctx", "tp"), None), P(None, "tp"), P(None, "tp"), P(), P()),
        out_specs=P("ctx", "tp"),
        check_vma=False,
    )
```
